32 devices in a mesh: head: 2 (over y), ctx: 16 (over z, x, core).
Axes of the slice: x: 2, y: 2, z: 4, core: 2. Of those that a mesh axis runs over, the one named last changes fastest.
Arguments:
- video_q: bfloat16 [4096, 2048], P('ctx', 'head'), may hold values from -8 to 8
- video_k: bfloat16 [4096, 2048], P('ctx', 'head'), may hold values from -8 to 8
- video_v: bfloat16 [4096, 2048], P('ctx', 'head'), may hold values from -6 to 6
- audio_q: bfloat16 [128, 2048], P('ctx', 'head'), may hold values from -8 to 8
- audio_k: bfloat16 [128, 2048], P('ctx', 'head'), may hold values from -8 to 8
- audio_v: bfloat16 [128, 2048], P('ctx', 'head'), may hold values from -6 to 6
- video_length: int32 [1], replicated, may hold values from 2048 to 4096
- video_cot: bfloat16 [16, 256, 2048], P('ctx', 'head'), may hold values from -6 to 6
- audio_cot: bfloat16 [128, 2048], P('ctx', 'head'), may hold values from -6 to 6
Outputs:
- video_out: bfloat16 [16, 256, 2048], P('ctx', 'head')
- audio_out: bfloat16 [128, 2048], P('ctx', 'head')
- grad_video_q: bfloat16 [4096, 2048], P('ctx', 'head')
- grad_video_k: bfloat16 [4096, 2048], P('ctx', 'head')
- grad_video_v: bfloat16 [4096, 2048], P('ctx', 'head')
- grad_audio_q: bfloat16 [128, 2048], P('ctx', 'head')
- grad_audio_k: bfloat16 [128, 2048], P('ctx', 'head')
- grad_audio_v: bfloat16 [128, 2048], P('ctx', 'head')
The draws below stay inside these ranges and needn't reach their ends.
All inputs are finite; a program needn't handle non-finite values.
Results may differ from the reference program's by a relative error of at most 0.011.
Values may be sent and summed in bfloat16 or wider, within the bound.
No kernel may reach another device: no remote copies, remote signals or barrier semaphores. Data moves between devices by JAX's collectives and lax.ppermute only.
A program may use at most 64 MiB of HBM per device.

```python
import jax
import jax.numpy as jnp
from jax import lax

HEADS = 32
HEAD_DIM = 64
VID_DEV = 256
VIDEO = 4096
AUDIO = 128
N_CTX = 16


def drawn_rows(key, salt, row_total):
    feat_total = HEADS * HEAD_DIM
    inner = jax.random.fold_in(key, salt)
    return jnp.clip(jax.random.normal(jax.random.fold_in(inner, 6), (row_total, feat_total)), -6.0, 6.0)


def drawn_queries(key, salt, row_total):
    drawn = drawn_rows(key, salt, row_total)
    return drawn


def drawn_keys(key, salt, row_total):
    drawn = drawn_rows(key, salt, row_total)
    return drawn


def draw_video_q(key, part):
    return drawn_queries(key, 11, VIDEO).astype(jnp.bfloat16)


def draw_audio_k(key, part):
    return drawn_keys(key, 12, AUDIO).astype(jnp.bfloat16)


def draw_audio_q(key, part):
    return drawn_queries(key, 13, AUDIO).astype(jnp.bfloat16)


def draw_video_k(key, part):
    return drawn_keys(key, 14, VIDEO).astype(jnp.bfloat16)


def block_scale(key, extent, shards, low, top_value):
    loudness = 1.0
    for position, shards_of in shards:
        steps = jax.random.uniform(jax.random.fold_in(jax.random.fold_in(key, 6), position), (shards_of,), jnp.float32, low / len(shards), top_value / len(shards))
        loudness = loudness * jnp.repeat(jnp.exp(steps), extent[position] // shards_of).reshape((-1,) + (1,) * (len(extent) - 1 - position))
    return loudness


def scatter_about(key, dims, width, reach, split=(), kind=jnp.bfloat16):
    entries = jax.random.normal(key, dims, jnp.float32) * width
    if len(split) > 0:
        entries = block_scale(key, dims, split, -0.22, 0.18) * entries
    return jnp.clip(entries, min=-reach, max=reach).astype(kind)


def setup_inputs(seed: int = 0) -> dict:
    seeds = jax.random.split(jax.random.key(seed), 10)
    return {
        "video_q": draw_video_q(jax.random.fold_in(seeds[9], 71), 0),
        "video_k": draw_video_k(jax.random.fold_in(seeds[9], 71), 0),
        "video_v": scatter_about(seeds[2], (VIDEO, HEADS * HEAD_DIM), 1.0, 6.0, ((0, 16), (1, 2))),
        "audio_q": draw_audio_q(jax.random.fold_in(seeds[9], 71), 0),
        "audio_k": draw_audio_k(jax.random.fold_in(seeds[9], 71), 0),
        "audio_v": scatter_about(seeds[5], (AUDIO, HEADS * HEAD_DIM), 1.0, 6.0, ((0, 16), (1, 2))),
        "video_length": jax.random.randint(seeds[6], (1,), VIDEO // 2, VIDEO + 1).astype(jnp.int32),
        "video_cot": scatter_about(seeds[7], (N_CTX, VID_DEV, HEADS * HEAD_DIM), 1.0, 6.0, ((0, 16), (1, 2))),
        "audio_cot": scatter_about(seeds[8], (AUDIO, HEADS * HEAD_DIM), 1.0, 6.0, ((0, 16), (1, 2))),
    }


def split_heads(matrix):
    return matrix.reshape(matrix.shape[0], HEADS, HEAD_DIM).transpose(1, 0, 2)


def join_heads(stacked):
    return stacked.transpose(1, 0, 2).reshape(stacked.shape[1], HEADS * HEAD_DIM)


def reference(video_q, video_k, video_v, audio_q, audio_k, audio_v, video_length, video_cot, audio_cot):
    score_scale = HEAD_DIM ** -0.5
    video_grad = video_cot.reshape(VIDEO, HEADS * HEAD_DIM)
    is_live = (lax.iota(jnp.int32, VIDEO) < video_length[0].astype(jnp.int32))[None, :]

    def per_head(operands):
        q_video, k_video, v_video, q_audio, k_audio, v_audio, g_video, g_audio = operands
        s_one = jnp.dot(q_video, k_audio.T, preferred_element_type=jnp.float32) * score_scale
        e_one = jnp.exp(s_one - jnp.max(s_one, axis=1, keepdims=True))
        p_one = e_one / jnp.sum(e_one, axis=1, keepdims=True)
        pb_one = p_one.astype(jnp.bfloat16)
        o_video = jnp.dot(pb_one, v_audio, preferred_element_type=jnp.float32)
        dp_one = jnp.dot(g_video, v_audio.T, preferred_element_type=jnp.float32)
        proj_one = jnp.sum(g_video.astype(jnp.float32) * o_video, axis=1, keepdims=True)
        ds_one = (score_scale * p_one * (dp_one - proj_one)).astype(jnp.bfloat16)
        dq_video = jnp.dot(ds_one, k_audio, preferred_element_type=jnp.float32)
        dk_audio = jnp.dot(ds_one.T, q_video, preferred_element_type=jnp.float32)
        dv_audio = jnp.dot(pb_one.T, g_video, preferred_element_type=jnp.float32)
        s_two = jnp.dot(q_audio, k_video.T, preferred_element_type=jnp.float32) * score_scale
        m_two = jnp.max(jnp.where(is_live, s_two, -1e30), axis=1, keepdims=True)
        e_two = jnp.where(is_live, jnp.exp(s_two - m_two), 0.0)
        l_two = jnp.sum(e_two, axis=1, keepdims=True)
        o_audio = jnp.dot(e_two.astype(jnp.bfloat16), v_video, preferred_element_type=jnp.float32) / l_two
        p_two = e_two / l_two
        dp_two = jnp.dot(g_audio, v_video.T, preferred_element_type=jnp.float32)
        proj_two = jnp.sum(g_audio.astype(jnp.float32) * o_audio, axis=1, keepdims=True)
        ds_two = (score_scale * p_two * (dp_two - proj_two)).astype(jnp.bfloat16)
        dq_audio = jnp.dot(ds_two, k_video, preferred_element_type=jnp.float32)
        dk_video = jnp.dot(ds_two.T, q_audio, preferred_element_type=jnp.float32)
        dv_video = jnp.dot(p_two.astype(jnp.bfloat16).T, g_audio, preferred_element_type=jnp.float32)
        return tuple(item.astype(jnp.bfloat16) for item in (o_video, o_audio, dq_video, dk_video, dv_video, dq_audio, dk_audio, dv_audio))

    inputs = tuple(split_heads(item) for item in (video_q, video_k, video_v, audio_q, audio_k, audio_v, video_grad, audio_cot))
    results = lax.map(per_head, inputs)
    joined = [join_heads(item) for item in results]
    video_out = joined[0].reshape(N_CTX, VID_DEV, HEADS * HEAD_DIM)
    return (video_out, joined[1], joined[2], joined[3], joined[4], joined[5], joined[6], joined[7])
```

```python
import functools

import jax
import jax.numpy as jnp
from jax import lax
from jax.experimental import pallas as pl
from jax.experimental.pallas import tpu as pltpu
from jax.sharding import PartitionSpec as P

HEAD_DIM = 64
PAIR = 2 * HEAD_DIM
SCALE = HEAD_DIM ** (-0.5)
NEG = -1e30
F32 = jnp.float32
BF16 = jnp.bfloat16


def nt(x, y):
    return lax.dot_general(x, y, (((1,), (1,)), ((), ())), preferred_element_type=F32)


def nn(x, y):
    return jnp.dot(x, y, preferred_element_type=F32)


def tn(x, y):
    return lax.dot_general(x, y, (((0,), (0,)), ((), ())), preferred_element_type=F32)


def first_head(shape):
    return lax.broadcasted_iota(jnp.int32, shape, len(shape) - 1) < HEAD_DIM


def block_diag(low, high):
    rows = jnp.concatenate([low, high], axis=0)
    keep = first_head(rows.shape)
    zero = jnp.zeros_like(rows)
    return jnp.concatenate([jnp.where(keep, rows, zero), jnp.where(keep, zero, rows)], axis=0)


def join_pair(stacked):
    rows = stacked.shape[0] // 2
    return jnp.where(first_head((rows, PAIR)), stacked[:rows], stacked[rows:])


def audio_kernel(live_ref, q_lo, q_hi, c_lo, c_hi, key_ref, val_ref, stat_ref, keep_ref, send_ref):
    keys, vals = key_ref[...], val_ref[...]
    queries = block_diag(q_lo[...], q_hi[...])
    cots = block_diag(c_lo[...], c_hi[...])
    rows = queries.shape[0] // 2
    scores = nt(queries, keys) * SCALE
    live = lax.broadcasted_iota(jnp.int32, scores.shape, 1) < live_ref[0]
    top = jnp.max(jnp.where(live, scores, NEG), axis=1, keepdims=True)
    weights = jnp.where(live, jnp.exp(scores - top), 0.0)
    total = jnp.sum(weights, axis=1, keepdims=True)
    dprob = nt(cots, vals)
    mean = jnp.sum(weights * dprob, axis=1, keepdims=True) / jnp.where(total > 0.0, total, 1.0)
    spread = (weights * (dprob - mean)).astype(BF16)
    rounded = weights.astype(BF16)
    parts = (
        join_pair(nn(rounded, vals)),
        join_pair(nn(spread, keys)),
        join_pair(nn(rounded, keys)),
    )
    half = rows // 2
    for index, part in enumerate(parts):
        keep_ref[index] = part[:half]
        send_ref[index] = part[half:].astype(BF16)
    lane = lax.broadcasted_iota(jnp.int32, (rows, PAIR), 1)
    table = jnp.zeros((rows, PAIR), F32)
    for index, column in enumerate((top, total, mean)):
        table = jnp.where(lane == 2 * index, column[:rows], table)
        table = jnp.where(lane == 2 * index + 1, column[rows:], table)
    stat_ref[0] = table.T[:8]


def video_kernel(k_lo, k_hi, v_lo, v_hi, query_ref, grad_ref, out_ref, dq_ref, keep_ref, send_ref):
    queries, grads = query_ref[...], grad_ref[...]
    keys = block_diag(k_lo[...], k_hi[...])
    vals = block_diag(v_lo[...], v_hi[...])
    rows = keys.shape[0] // 2
    scores = nt(queries, keys) * SCALE
    probs = []
    for part in (scores[:, :rows], scores[:, rows:]):
        shifted = jnp.exp(part - jnp.max(part, axis=1, keepdims=True))
        probs.append(shifted / jnp.sum(shifted, axis=1, keepdims=True))
    rounded = jnp.concatenate([prob.astype(BF16) for prob in probs], axis=1)
    attended = nn(rounded, vals)
    out_ref[...] = attended.astype(BF16)
    dprob = nt(grads, vals)
    product = grads.astype(F32) * attended
    low = first_head(product.shape)
    proj = (
        jnp.sum(jnp.where(low, product, 0.0), axis=1, keepdims=True),
        jnp.sum(jnp.where(low, 0.0, product), axis=1, keepdims=True),
    )
    steps = jnp.concatenate(
        [
            (SCALE * probs[h] * (dprob[:, h * rows : (h + 1) * rows] - proj[h])).astype(BF16)
            for h in range(2)
        ],
        axis=1,
    )
    dq_ref[...] = nn(steps, keys).astype(BF16)
    half = rows // 2
    for index, part in enumerate((join_pair(tn(steps, queries)), join_pair(tn(rounded, grads)))):
        keep_ref[index] = part[:half]
        send_ref[index] = part[half:].astype(BF16)


def swap_lanes(x, shift):
    size = x.shape[-1]
    lane = lax.broadcasted_iota(jnp.int32, x.shape, x.ndim - 1)
    up = pltpu.roll(x, size - shift, x.ndim - 1)
    down = pltpu.roll(x, shift, x.ndim - 1)
    return jnp.where((lane & shift) == 0, up, down)


def merge_stats(mine, other, shift):
    other = swap_lanes(other, shift)
    top1, total1, mean1 = mine[0:2], mine[2:4], mine[4:6]
    top2, total2, mean2 = other[0:2], other[2:4], other[4:6]
    top = jnp.maximum(top1, top2)
    scale1, scale2 = jnp.exp(top1 - top), jnp.exp(top2 - top)
    part1, part2 = scale1 * total1, scale2 * total2
    total = part1 + part2
    mean = (part1 * mean1 + part2 * mean2) / jnp.where(total > 0.0, total, 1.0)
    shift1, shift2 = scale1 * (mean1 - mean), scale2 * (mean2 - mean)
    return top, total, mean, scale1, scale2, shift1, shift2


def merge_kernel(n_in, last, shift, *refs):
    mine_ref, other_ref = refs[:2]
    keeps, recvs = refs[2 : 2 + n_in], refs[2 + n_in : 2 + 2 * n_in]
    outs = refs[2 + 2 * n_in :]
    pairs, _, lanes = mine_ref.shape
    rows = keeps[0].shape[1]
    tables = []
    for pair in range(pairs):
        top, total, mean, scale1, scale2, shift1, shift2 = merge_stats(
            mine_ref[pair], other_ref[pair], shift
        )
        if last:
            inverse = 1.0 / total
            tables += [scale1 * inverse, scale2 * inverse, shift1 * inverse, shift2 * inverse]
        else:
            tables += [scale1, scale2, shift1, shift2]
            pad = jnp.zeros_like(top)
            outs[2][pair] = jnp.concatenate([top, total, mean, pad], axis=0)
    table = jnp.concatenate(tables, axis=0)
    if table.shape[0] < 128:
        table = jnp.concatenate([table, jnp.zeros((128 - table.shape[0], lanes), F32)], axis=0)
    table = table.T
    low = first_head((rows, PAIR))

    def fetch(group, index, cols):
        for ref in group:
            if index < ref.shape[0]:
                return ref[index, :, cols].astype(F32)
            index -= ref.shape[0]

    for pair in range(pairs):
        cols = slice(pair * PAIR, (pair + 1) * PAIR)

        def column(index):
            at = pair * 8 + 2 * index
            return jnp.where(low, table[:rows, at : at + 1], table[:rows, at + 1 : at + 2])

        scale1, scale2, shift1, shift2 = (column(index) for index in range(4))
        num1, step1, sum1, key1, val1 = (fetch(keeps, index, cols) for index in range(5))
        num2, step2, sum2, key2, val2 = (fetch(recvs, index, cols) for index in range(5))
        num = scale1 * num1 + scale2 * num2
        step = scale1 * step1 + shift1 * sum1 + scale2 * step2 + shift2 * sum2
        key, val = key1 + key2, val1 + val2
        if last:
            outs[0][:, cols] = num.astype(BF16)
            outs[1][:, cols] = (SCALE * step).astype(BF16)
            outs[2][:, cols] = key.astype(BF16)
            outs[3][:, cols] = val.astype(BF16)
        else:
            total = scale1 * sum1 + scale2 * sum2
            half = rows // 2
            for index, part in enumerate((num, step, total, key, val)):
                outs[0][index, :, cols] = part[:half]
                outs[1][index, :, cols] = part[half:].astype(BF16)


def final_kernel(shift, live_ref, q_lo, q_hi, c_lo, c_hi, key_ref, val_ref, mine_ref, other_ref, dk_ref, dv_ref):
    keys, vals = key_ref[...], val_ref[...]
    queries = block_diag(q_lo[...], q_hi[...])
    cots = block_diag(c_lo[...], c_hi[...])
    top, total, mean = merge_stats(mine_ref[0], other_ref[0], shift)[:3]
    inverse = 1.0 / total
    top, inverse, mean = (
        jnp.concatenate([item[0:1], item[1:2]], axis=1) for item in (top, inverse, mean)
    )
    scores = nt(keys, queries) * SCALE
    live = lax.broadcasted_iota(jnp.int32, scores.shape, 0) < live_ref[0]
    probs = jnp.where(live, jnp.exp(scores - top), 0.0) * inverse
    dprob = nt(vals, cots)
    steps = (SCALE * probs * (dprob - mean)).astype(BF16)
    dk_ref[...] = nn(steps, queries).astype(BF16)
    dv_ref[...] = nn(probs.astype(BF16), cots).astype(BF16)


def body(video_q, video_k, video_v, audio_q, audio_k, audio_v, video_length, video_cot, audio_cot):
    vid_rows, width = video_q.shape
    aud_rows = audio_q.shape[0]
    ctx_size, head_size = lax.axis_size("ctx"), lax.axis_size("head")
    ctx_index, head_index = lax.axis_index("ctx"), lax.axis_index("head")
    rows = aud_rows * ctx_size
    half = rows // 2
    pairs = width // PAIR
    bits = []
    while (1 << len(bits)) < ctx_size:
        bits.append(1 << len(bits))
    live = jnp.clip(video_length - ctx_index * vid_rows, 0, vid_rows).astype(jnp.int32)

    def flip(x, bit):
        return lax.ppermute(x, "ctx", [(i, i ^ bit) for i in range(ctx_size)])

    cot = video_cot[0]
    tok_rows = cot.shape[0]
    if head_size == 2:
        sent = lax.dynamic_slice_in_dim(cot, (1 - head_index) * width, width, 1)
        kept = lax.dynamic_slice_in_dim(cot, head_index * width, width, 1)
        got = lax.ppermute(sent, "head", [(0, 1), (1, 0)])
        video_grad = jnp.concatenate(
            [jnp.where(head_index == 0, kept, got), jnp.where(head_index == 0, got, kept)], axis=0
        )
    else:
        video_grad = lax.all_to_all(cot, "head", split_axis=1, concat_axis=0, tiled=True)

    gathered = jnp.concatenate([audio_q, audio_k, audio_v, audio_cot], axis=1)
    for bit in reversed(bits[1:]):
        gathered = jnp.concatenate([gathered, flip(gathered, bit)], axis=0)
    halves = (gathered, flip(gathered, bits[0]))

    def audio_spec(which):
        return pl.BlockSpec((half, PAIR), lambda pair: (0, which * pairs + pair))

    vid_spec = pl.BlockSpec((vid_rows, PAIR), lambda pair: (0, pair))
    scalar_spec = pl.BlockSpec(memory_space=pltpu.SMEM)
    stat_spec = pl.BlockSpec((1, 8, rows), lambda pair: (pair, 0, 0))
    stat_shape = jax.ShapeDtypeStruct((pairs, 8, rows), F32)

    def part_spec(count):
        return pl.BlockSpec((count, half, PAIR), lambda pair: (0, 0, pair))

    def part_shapes(count, part_rows):
        return [
            jax.ShapeDtypeStruct((count, part_rows, width), F32),
            jax.ShapeDtypeStruct((count, part_rows, width), BF16),
        ]

    product = 2 * vid_rows * 2 * rows * PAIR * pairs
    vid_bytes = 2 * vid_rows * width
    vid_shape = jax.ShapeDtypeStruct((vid_rows, width), BF16)

    def cost(matmuls, moved):
        return pl.CostEstimate(
            flops=matmuls * product, bytes_accessed=moved * vid_bytes, transcendentals=vid_rows * 2 * rows * pairs
        )

    stats, keep_a, send_a = pl.pallas_call(
        audio_kernel,
        grid=(pairs,),
        in_specs=[scalar_spec, audio_spec(0), audio_spec(0), audio_spec(3), audio_spec(3), vid_spec, vid_spec],
        out_specs=[stat_spec, part_spec(3), part_spec(3)],
        out_shape=[stat_shape, *part_shapes(3, half)],
        cost_estimate=cost(5, 5),
        name="audio_side",
    )(live, *halves, *halves, video_k, video_v)

    video_attended, grad_video_q, keep_b, send_b = pl.pallas_call(
        video_kernel,
        grid=(pairs,),
        in_specs=[audio_spec(1), audio_spec(1), audio_spec(2), audio_spec(2), vid_spec, vid_spec],
        out_specs=[vid_spec, vid_spec, part_spec(2), part_spec(2)],
        out_shape=[vid_shape, vid_shape, *part_shapes(2, half)],
        cost_estimate=cost(6, 6),
        name="video_side",
    )(*halves, *halves, video_q, video_grad)

    if head_size == 2:
        mine = lax.dynamic_slice_in_dim(video_attended, head_index * tok_rows, tok_rows, 0)
        theirs = lax.dynamic_slice_in_dim(video_attended, (1 - head_index) * tok_rows, tok_rows, 0)
        other = lax.ppermute(theirs, "head", [(0, 1), (1, 0)])
        video_out = jnp.concatenate(
            [jnp.where(head_index == 0, mine, other), jnp.where(head_index == 0, other, mine)], axis=1
        )[None]
    else:
        video_out = lax.all_to_all(video_attended, "head", split_axis=0, concat_axis=1, tiled=True)[None]

    keeps, sends = (keep_a, keep_b), (send_a, send_b)
    part_rows = half
    for bit in bits:
        last = bit == bits[-1]
        other_stats = flip(stats, bit)
        recvs = tuple(flip(send, bit) for send in sends)
        if last:
            out_shape = [jax.ShapeDtypeStruct((part_rows, width), BF16)] * 4
        else:
            out_shape = [*part_shapes(5, part_rows // 2), stat_shape]
        merged = pl.pallas_call(
            functools.partial(merge_kernel, len(keeps), last, part_rows),
            out_shape=out_shape,
            name=f"merge_{bit}",
        )(stats, other_stats, *keeps, *recvs)
        if last:
            audio_out, grad_audio_q, grad_audio_k, grad_audio_v = merged
        else:
            keep, send, stats = merged
            keeps, sends = (keep,), (send,)
            part_rows //= 2

    grad_video_k, grad_video_v = pl.pallas_call(
        functools.partial(final_kernel, part_rows),
        grid=(pairs,),
        in_specs=[
            scalar_spec,
            audio_spec(0),
            audio_spec(0),
            audio_spec(3),
            audio_spec(3),
            vid_spec,
            vid_spec,
            stat_spec,
            stat_spec,
        ],
        out_specs=[vid_spec, vid_spec],
        out_shape=[vid_shape, vid_shape],
        cost_estimate=cost(4, 4),
        name="audio_grads",
    )(live, *halves, *halves, video_k, video_v, stats, other_stats)
    return (
        video_out,
        audio_out,
        grad_video_q,
        grad_video_k,
        grad_video_v,
        grad_audio_q,
        grad_audio_k,
        grad_audio_v,
    )


def solution(mesh):
    wide = P("ctx", "head")
    tall = P("ctx", "head", None)
    return jax.shard_map(
        body,
        mesh=mesh,
        in_specs=(wide, wide, wide, wide, wide, wide, P(), tall, wide),
        out_specs=(tall, wide, wide, wide, wide, wide, wide, wide),
        check_vma=False,
    )
```

```python
import functools

import jax
import jax.numpy as jnp
from jax import lax
from jax.experimental import pallas as pl
from jax.experimental.pallas import tpu as pltpu
from jax.sharding import PartitionSpec as P


HEAD_DIM = 64
PAIR = 2 * HEAD_DIM
SCALE = HEAD_DIM ** (-0.5)
NEG = -1e30
GROUP = 2
PARAMS = pltpu.CompilerParams(vmem_limit_bytes=12 * 1024 * 1024)
F32 = jnp.float32
BF16 = jnp.bfloat16


def nt(x, y):
    return lax.dot_general(x, y, (((1,), (1,)), ((), ())), preferred_element_type=F32)


def nn(x, y):
    return jnp.dot(x, y, preferred_element_type=F32)


def tn(x, y):
    return lax.dot_general(x, y, (((0,), (0,)), ((), ())), preferred_element_type=F32)


def first_head(shape):
    return lax.broadcasted_iota(jnp.int32, shape, len(shape) - 1) < HEAD_DIM


def block_diag(low, high):
    rows = jnp.concatenate([low, high], axis=0)
    keep = first_head(rows.shape)
    zero = jnp.zeros_like(rows)
    return jnp.concatenate([jnp.where(keep, rows, zero), jnp.where(keep, zero, rows)], axis=0)


def join_pair(stacked):
    rows = stacked.shape[0] // 2
    return jnp.where(first_head((rows, PAIR)), stacked[:rows], stacked[rows:])


def pair_cols(pair):
    return slice(pair * PAIR, (pair + 1) * PAIR)


def audio_kernel(live_ref, q_lo, q_hi, c_lo, c_hi, key_ref, val_ref, stat_ref, keep_ref, send_ref):
    for pair in range(stat_ref.shape[0]):
        cols = pair_cols(pair)
        keys, vals = key_ref[:, cols], val_ref[:, cols]
        queries = block_diag(q_lo[:, cols], q_hi[:, cols])
        cots = block_diag(c_lo[:, cols], c_hi[:, cols])
        rows = queries.shape[0] // 2
        scores = nt(queries, keys) * SCALE
        live = lax.broadcasted_iota(jnp.int32, scores.shape, 1) < live_ref[0]
        top = jnp.max(jnp.where(live, scores, NEG), axis=1, keepdims=True)
        weights = jnp.where(live, jnp.exp(scores - top), 0.0)
        total = jnp.sum(weights, axis=1, keepdims=True)
        dprob = nt(cots, vals)
        mean = jnp.sum(weights * dprob, axis=1, keepdims=True) / jnp.where(total > 0.0, total, 1.0)
        spread = (weights * (dprob - mean)).astype(BF16)
        rounded = weights.astype(BF16)
        parts = (
            join_pair(nn(rounded, vals)),
            join_pair(nn(spread, keys)),
            join_pair(nn(rounded, keys)),
        )
        half = rows // 2
        for index, part in enumerate(parts):
            keep_ref[index, :, cols] = part[:half]
            send_ref[index, :, cols] = part[half:].astype(BF16)
        lane = lax.broadcasted_iota(jnp.int32, (rows, PAIR), 1)
        table = jnp.zeros((rows, PAIR), F32)
        for index, column in enumerate((top, total, mean)):
            table = jnp.where(lane == 2 * index, column[:rows], table)
            table = jnp.where(lane == 2 * index + 1, column[rows:], table)
        stat_ref[pair] = table.T[:8]


def video_kernel(head_ref, k_lo, k_hi, v_lo, v_hi, query_ref, grad_ref, *outs):
    *out_refs, dq_ref, keep_ref, send_ref = outs
    for pair in range(query_ref.shape[1] // PAIR):
        cols = pair_cols(pair)
        queries, grads = query_ref[:, cols], grad_ref[:, cols]
        keys = block_diag(k_lo[:, cols], k_hi[:, cols])
        vals = block_diag(v_lo[:, cols], v_hi[:, cols])
        rows = keys.shape[0] // 2
        scores = nt(queries, keys) * SCALE
        probs = []
        for part in (scores[:, :rows], scores[:, rows:]):
            shifted = jnp.exp(part - jnp.max(part, axis=1, keepdims=True))
            probs.append(shifted * (1.0 / jnp.sum(shifted, axis=1, keepdims=True)))
        rounded = jnp.concatenate([prob.astype(BF16) for prob in probs], axis=1)
        attended = nn(rounded, vals)
        if len(out_refs) == 1:
            out_refs[0][:, cols] = attended.astype(BF16)
        else:
            tok_rows = attended.shape[0] // 2
            upper, lower = attended[:tok_rows].astype(BF16), attended[tok_rows:].astype(BF16)
            is_first = jnp.full(upper.shape, head_ref[0], jnp.int32) == 0
            out_refs[0][:, cols] = jnp.where(is_first, upper, lower)
            out_refs[1][:, cols] = jnp.where(is_first, lower, upper)
        dprob = nt(grads, vals)
        product = grads.astype(F32) * attended
        low = first_head(product.shape)
        proj = (
            jnp.sum(jnp.where(low, product, 0.0), axis=1, keepdims=True),
            jnp.sum(jnp.where(low, 0.0, product), axis=1, keepdims=True),
        )
        steps = jnp.concatenate(
            [
                (SCALE * probs[h] * (dprob[:, h * rows : (h + 1) * rows] - proj[h])).astype(BF16)
                for h in range(2)
            ],
            axis=1,
        )
        dq_ref[:, cols] = nn(steps, keys).astype(BF16)
        half = rows // 2
        for index, part in enumerate((join_pair(tn(steps, queries)), join_pair(tn(rounded, grads)))):
            keep_ref[index, :, cols] = part[:half]
            send_ref[index, :, cols] = part[half:].astype(BF16)


def swap_lanes(x, shift):
    size = x.shape[-1]
    lane = lax.broadcasted_iota(jnp.int32, x.shape, x.ndim - 1)
    up = pltpu.roll(x, size - shift, x.ndim - 1)
    down = pltpu.roll(x, shift, x.ndim - 1)
    return jnp.where((lane & shift) == 0, up, down)


def merge_stats(mine, other, shift):
    other = swap_lanes(other, shift)
    top1, total1, mean1 = mine[0:2], mine[2:4], mine[4:6]
    top2, total2, mean2 = other[0:2], other[2:4], other[4:6]
    top = jnp.maximum(top1, top2)
    scale1, scale2 = jnp.exp(top1 - top), jnp.exp(top2 - top)
    part1, part2 = scale1 * total1, scale2 * total2
    total = part1 + part2
    mean = (part1 * mean1 + part2 * mean2) / jnp.where(total > 0.0, total, 1.0)
    shift1, shift2 = scale1 * (mean1 - mean), scale2 * (mean2 - mean)
    return top, total, mean, scale1, scale2, shift1, shift2


def stats_kernel(shift, mine_ref, other_ref, out_ref):
    for pair in range(mine_ref.shape[0]):
        top, total, mean = merge_stats(mine_ref[pair], other_ref[pair], shift)[:3]
        out_ref[pair] = jnp.concatenate([top, total, mean, jnp.zeros_like(top)], axis=0)


def merge_tables(pairs, factors):
    tables = []
    for pair in range(pairs):
        tables += factors(pair)
    table = jnp.concatenate(tables, axis=0)
    if table.shape[0] < 128:
        pad = jnp.zeros((128 - table.shape[0], table.shape[1]), F32)
        table = jnp.concatenate([table, pad], axis=0)
    return table.T


def merged_parts(table, pair, keeps, recvs):
    cols = pair_cols(pair)
    rows = keeps[0].shape[1]
    low = first_head((rows, PAIR))

    def column(index):
        at = pair * 8 + 2 * index
        return jnp.where(low, table[:rows, at : at + 1], table[:rows, at + 1 : at + 2])

    def fetch(group, index):
        for ref in group:
            if index < ref.shape[0]:
                return ref[index, :, cols].astype(F32)
            index -= ref.shape[0]

    scale1, scale2, shift1, shift2 = (column(index) for index in range(4))
    num1, step1, sum1, key1, val1 = (fetch(keeps, index) for index in range(5))
    num2, step2, sum2, key2, val2 = (fetch(recvs, index) for index in range(5))
    num = scale1 * num1 + scale2 * num2
    step = scale1 * step1 + shift1 * sum1 + scale2 * step2 + shift2 * sum2
    return num, step, scale1 * sum1 + scale2 * sum2, key1 + key2, val1 + val2


def merge_kernel(n_in, shift, *refs):
    mine_ref, other_ref = refs[:2]
    keeps, recvs = refs[2 : 2 + n_in], refs[2 + n_in : 2 + 2 * n_in]
    keep_ref, send_ref = refs[2 + 2 * n_in :]
    pairs = mine_ref.shape[0]
    half = keeps[0].shape[1] // 2
    table = merge_tables(
        pairs, lambda pair: list(merge_stats(mine_ref[pair], other_ref[pair], shift)[3:])
    )
    for pair in range(pairs):
        cols = pair_cols(pair)
        for index, part in enumerate(merged_parts(table, pair, keeps, recvs)):
            keep_ref[index, :, cols] = part[:half]
            send_ref[index, :, cols] = part[half:].astype(BF16)


def settle_kernel(n_in, shift, *refs):
    mine_ref, other_ref, all_ref = refs[:3]
    keeps, recvs = refs[3 : 3 + n_in], refs[3 + n_in : 3 + 2 * n_in]
    outs = refs[3 + 2 * n_in :]
    pairs = mine_ref.shape[0]
    rows = outs[0].shape[1]

    def factors(pair):
        both = all_ref[pair]
        top, inverse, mean = both[0:2], 1.0 / both[2:4], both[4:6]
        mine, other = mine_ref[pair], swap_lanes(other_ref[pair], shift)
        scales = [jnp.exp(item[0:2] - top) * inverse for item in (mine, other)]
        return scales + [
            scale * (item[4:6] - mean) for scale, item in zip(scales, (mine, other))
        ]

    table = merge_tables(pairs, factors)
    for pair in range(pairs):
        cols = pair_cols(pair)
        num, step, _, key, val = merged_parts(table, pair, keeps, recvs)
        for index, part in enumerate((num, SCALE * step, key, val)):
            for slot, out in enumerate(outs):
                out[index, :, cols] = part[slot * rows : (slot + 1) * rows].astype(out.dtype)


def add_kernel(*refs):
    parts, outs = refs[:-4], refs[-4:]
    for index, out in enumerate(outs):
        total = parts[0][index].astype(F32)
        for part in parts[1:]:
            total = total + part[index].astype(F32)
        out[...] = total.astype(BF16)


def final_kernel(live_ref, q_lo, q_hi, c_lo, c_hi, key_ref, val_ref, stat_ref, dk_ref, dv_ref):
    for pair in range(stat_ref.shape[0]):
        cols = pair_cols(pair)
        keys, vals = key_ref[:, cols], val_ref[:, cols]
        queries = block_diag(q_lo[:, cols], q_hi[:, cols])
        cots = block_diag(c_lo[:, cols], c_hi[:, cols])
        stat = stat_ref[pair]
        top, inverse, mean = stat[0:2], 1.0 / stat[2:4], stat[4:6]
        top, inverse, mean = (
            jnp.concatenate([item[0:1], item[1:2]], axis=1) for item in (top, inverse, mean)
        )
        scores = nt(keys, queries) * SCALE
        live = lax.broadcasted_iota(jnp.int32, scores.shape, 0) < live_ref[0]
        probs = jnp.where(live, jnp.exp(scores - top), 0.0) * inverse
        dprob = nt(vals, cots)
        steps = (SCALE * probs * (dprob - mean)).astype(BF16)
        dk_ref[:, cols] = nn(steps, queries).astype(BF16)
        dv_ref[:, cols] = nn(probs.astype(BF16), cots).astype(BF16)


def pack_kernel(*refs):
    width = refs[0].shape[1]
    for index, ref in enumerate(refs[:-1]):
        refs[-1][:, index * width : (index + 1) * width] = ref[...]


def body(video_q, video_k, video_v, audio_q, audio_k, audio_v, video_length, video_cot, audio_cot):
    vid_rows, width = video_q.shape
    aud_rows = audio_q.shape[0]
    ctx_size, head_size = lax.axis_size("ctx"), lax.axis_size("head")
    ctx_index, head_index = lax.axis_index("ctx"), lax.axis_index("head")
    rows = aud_rows * ctx_size
    half = rows // 2
    pairs = width // PAIR
    group = min(GROUP, pairs)
    steps = pairs // group
    wide = group * PAIR
    bits = []
    while (1 << len(bits)) < ctx_size:
        bits.append(1 << len(bits))
    live = jnp.clip(video_length - ctx_index * vid_rows, 0, vid_rows).astype(jnp.int32)

    def flip(x, bit):
        return lax.ppermute(x, "ctx", [(i, i ^ bit) for i in range(ctx_size)])

    cot = video_cot[0]
    tok_rows = cot.shape[0]
    if head_size == 2:
        sent = lax.dynamic_slice_in_dim(cot, (1 - head_index) * width, width, 1)
        kept = lax.dynamic_slice_in_dim(cot, head_index * width, width, 1)
        got = lax.ppermute(sent, "head", [(0, 1), (1, 0)])
        video_grad = jnp.concatenate(
            [jnp.where(head_index == 0, kept, got), jnp.where(head_index == 0, got, kept)], axis=0
        )
    else:
        video_grad = lax.all_to_all(cot, "head", split_axis=1, concat_axis=0, tiled=True)

    gathered = pl.pallas_call(
        pack_kernel,
        out_shape=jax.ShapeDtypeStruct((aud_rows, 4 * width), BF16),
        compiler_params=PARAMS,
        name="pack",
    )(audio_q, audio_k, audio_v, audio_cot)
    quarters = [gathered]
    for bit in (bits[-1], bits[-2], bits[-1] | bits[-2]):
        quarters.append(flip(gathered, bit))
    gathered = jnp.concatenate(quarters, axis=0)
    for bit in reversed(bits[1:-2]):
        got_rows = flip(gathered, bit)
        gathered = jnp.concatenate([gathered, got_rows], axis=0)
    halves = (gathered, flip(gathered, bits[0]))

    def audio_spec(which):
        return pl.BlockSpec((half, wide), lambda step: (0, which * steps + step))

    vid_spec = pl.BlockSpec((vid_rows, wide), lambda step: (0, step))
    scalar_spec = pl.BlockSpec(memory_space=pltpu.SMEM)
    stat_spec = pl.BlockSpec((group, 8, rows), lambda step: (step, 0, 0))
    stat_shape = jax.ShapeDtypeStruct((pairs, 8, rows), F32)

    def part_spec(count):
        return pl.BlockSpec((count, half, wide), lambda step: (0, 0, step))

    def part_shapes(count, part_rows):
        return [
            jax.ShapeDtypeStruct((count, part_rows, width), F32),
            jax.ShapeDtypeStruct((count, part_rows, width), BF16),
        ]

    product = 2 * vid_rows * 2 * rows * PAIR * pairs
    vid_bytes = 2 * vid_rows * width
    vid_shape = jax.ShapeDtypeStruct((vid_rows, width), BF16)

    def cost(matmuls, moved):
        return pl.CostEstimate(
            flops=matmuls * product, bytes_accessed=moved * vid_bytes, transcendentals=vid_rows * 2 * rows * pairs
        )

    stats, keep_a, send_a = pl.pallas_call(
        audio_kernel,
        grid=(steps,),
        compiler_params=PARAMS,
        in_specs=[scalar_spec, audio_spec(0), audio_spec(0), audio_spec(3), audio_spec(3), vid_spec, vid_spec],
        out_specs=[stat_spec, part_spec(3), part_spec(3)],
        out_shape=[stat_shape, *part_shapes(3, half)],
        cost_estimate=cost(5, 5),
        name="audio_side",
    )(live, *halves, *halves, video_k, video_v)

    if head_size == 2:
        tok_spec = pl.BlockSpec((tok_rows, wide), lambda step: (0, step))
        out_specs = [tok_spec, tok_spec]
        out_shapes = [jax.ShapeDtypeStruct((tok_rows, width), BF16)] * 2
    else:
        out_specs, out_shapes = [vid_spec], [vid_shape]
    *attended, grad_video_q, keep_b, send_b = pl.pallas_call(
        video_kernel,
        grid=(steps,),
        compiler_params=PARAMS,
        in_specs=[scalar_spec, audio_spec(1), audio_spec(1), audio_spec(2), audio_spec(2), vid_spec, vid_spec],
        out_specs=[*out_specs, vid_spec, part_spec(2), part_spec(2)],
        out_shape=[*out_shapes, vid_shape, *part_shapes(2, half)],
        cost_estimate=cost(6, 6),
        name="video_side",
    )(head_index.astype(jnp.int32)[None], *halves, *halves, video_q, video_grad)

    if head_size == 2:
        mine, theirs = attended
        other = lax.ppermute(theirs, "head", [(0, 1), (1, 0)])
        video_out = jnp.concatenate(
            [jnp.where(head_index == 0, mine, other), jnp.where(head_index == 0, other, mine)], axis=1
        )[None]
    else:
        video_out = lax.all_to_all(attended[0], "head", split_axis=0, concat_axis=1, tiled=True)[None]

    levels = [stats]
    others = []
    shift = half
    for bit in bits:
        others.append(flip(levels[-1], bit))
        levels.append(
            pl.pallas_call(
                functools.partial(stats_kernel, shift), out_shape=stat_shape, compiler_params=PARAMS
            )(levels[-1], others[-1])
        )
        shift //= 2

    keeps, sends = (keep_a, keep_b), (send_a, send_b)
    part_rows = half
    for level, bit in enumerate(bits[:-2]):
        recvs = []
        for send in sends:
            recvs.append(flip(send, bit))
        if level < len(bits) - 3:
            keep, send = pl.pallas_call(
                functools.partial(merge_kernel, len(keeps), part_rows),
                out_shape=part_shapes(5, part_rows // 2),
                compiler_params=PARAMS,
            )(levels[level], others[level], *keeps, *recvs)
            keeps, sends = (keep,), (send,)
            part_rows //= 2
        else:
            slots = pl.pallas_call(
                functools.partial(settle_kernel, len(keeps), part_rows),
                out_shape=[jax.ShapeDtypeStruct((4, aud_rows, width), dtype) for dtype in (F32, BF16, BF16, BF16)],
                compiler_params=PARAMS,
                name="settle",
            )(levels[level], others[level], levels[-1], *keeps, *recvs)
    high, low = bits[-1], bits[-2]
    parts = [slots[0]]
    for bit, slot in zip((high, low, high | low), slots[1:]):
        parts.append(flip(slot, bit))
    audio_out, grad_audio_q, grad_audio_k, grad_audio_v = pl.pallas_call(
        add_kernel,
        out_shape=[jax.ShapeDtypeStruct((aud_rows, width), BF16)] * 4,
        compiler_params=PARAMS,
        name="add",
    )(*parts)

    grad_video_k, grad_video_v = pl.pallas_call(
        final_kernel,
        grid=(steps,),
        compiler_params=PARAMS,
        in_specs=[
            scalar_spec,
            audio_spec(0),
            audio_spec(0),
            audio_spec(3),
            audio_spec(3),
            vid_spec,
            vid_spec,
            stat_spec,
        ],
        out_specs=[vid_spec, vid_spec],
        out_shape=[vid_shape, vid_shape],
        cost_estimate=cost(4, 4),
        name="audio_grads",
    )(live, *halves, *halves, video_k, video_v, levels[-1])
    return (
        video_out,
        audio_out,
        grad_video_q,
        grad_video_k,
        grad_video_v,
        grad_audio_q,
        grad_audio_k,
        grad_audio_v,
    )


def solution(mesh):
    wide = P("ctx", "head")
    tall = P("ctx", "head", None)

    return jax.shard_map(
        body,
        mesh=mesh,
        in_specs=(wide, wide, wide, wide, wide, wide, P(), tall, wide),
        out_specs=(tall, wide, wide, wide, wide, wide, wide, wide),
        check_vma=False,
    )
```

```python
import functools

import jax
import jax.numpy as jnp
from jax import lax
from jax.experimental import pallas as pl
from jax.experimental.pallas import tpu as pltpu
from jax.sharding import PartitionSpec as P


HEAD_DIM = 64
PAIR = 2 * HEAD_DIM
SCALE = HEAD_DIM ** (-0.5)
NEG = -1e30
GROUP = 4
PARAMS = pltpu.CompilerParams(vmem_limit_bytes=12 * 1024 * 1024)
F32 = jnp.float32
BF16 = jnp.bfloat16


def nt(x, y):
    return lax.dot_general(x, y, (((1,), (1,)), ((), ())), preferred_element_type=F32)


def nn(x, y):
    return jnp.dot(x, y, preferred_element_type=F32)


def first_head(shape):
    return lax.broadcasted_iota(jnp.int32, shape, len(shape) - 1) < HEAD_DIM


def block_diag(low, high):
    rows = jnp.concatenate([low, high], axis=0)
    keep = first_head(rows.shape)
    zero = jnp.zeros_like(rows)
    return jnp.concatenate([jnp.where(keep, rows, zero), jnp.where(keep, zero, rows)], axis=0)


def join_pair(stacked):
    rows = stacked.shape[0] // 2
    return jnp.where(first_head((rows, PAIR)), stacked[:rows], stacked[rows:])


def pair_cols(pair):
    return slice(pair * PAIR, (pair + 1) * PAIR)


def audio_kernel(live_ref, q_lo, q_hi, c_lo, c_hi, key_ref, val_ref, stat_ref, keep_ref, send_ref):
    for pair in range(stat_ref.shape[0]):
        cols = pair_cols(pair)
        keys, vals = key_ref[:, cols], val_ref[:, cols]
        queries = block_diag(q_lo[:, cols], q_hi[:, cols])
        cots = block_diag(c_lo[:, cols], c_hi[:, cols])
        rows = queries.shape[0] // 2
        scores = nt(queries, keys) * SCALE
        live = lax.broadcasted_iota(jnp.int32, scores.shape, 1) < live_ref[0]
        top = jnp.max(jnp.where(live, scores, NEG), axis=1, keepdims=True)
        weights = jnp.where(live, jnp.exp(scores - top), 0.0)
        total = jnp.sum(weights, axis=1, keepdims=True)
        dprob = nt(cots, vals)
        mean = jnp.sum(weights * dprob, axis=1, keepdims=True) / jnp.where(total > 0.0, total, 1.0)
        spread = (weights * (dprob - mean)).astype(BF16)
        rounded = weights.astype(BF16)
        parts = (
            join_pair(nn(rounded, vals)),
            join_pair(nn(spread, keys)),
            join_pair(nn(rounded, keys)),
        )
        half = rows // 2
        for index, part in enumerate(parts):
            keep_ref[index, :, cols] = part[:half]
            send_ref[index, :, cols] = part[half:].astype(BF16)
        lane = lax.broadcasted_iota(jnp.int32, (rows, PAIR), 1)
        table = jnp.zeros((rows, PAIR), F32)
        for index, column in enumerate((top, total, mean)):
            table = jnp.where(lane == 2 * index, column[:rows], table)
            table = jnp.where(lane == 2 * index + 1, column[rows:], table)
        stat_ref[pair] = table.T[:8]


def transposed_diag(low, high):
    turned = jnp.concatenate([low, high], axis=0).T
    keep = lax.broadcasted_iota(jnp.int32, turned.shape, 0) < HEAD_DIM
    zero = jnp.zeros_like(turned)
    return jnp.concatenate([jnp.where(keep, turned, zero), jnp.where(keep, zero, turned)], axis=1)


def video_kernel(head_ref, k_lo, k_hi, v_lo, v_hi, query_ref, grad_ref, *outs):
    *out_refs, dq_ref, keep_ref, send_ref = outs
    for pair in range(query_ref.shape[1] // PAIR):
        cols = pair_cols(pair)
        queries, grads = query_ref[:, cols], grad_ref[:, cols]
        keys = block_diag(k_lo[:, cols], k_hi[:, cols])
        vals = block_diag(v_lo[:, cols], v_hi[:, cols])
        rows = keys.shape[0] // 2
        scores = nt(keys, queries) * SCALE
        dprob = nt(vals, grads)
        probs, steps = [], []
        for head in range(2):
            span = slice(head * rows, (head + 1) * rows)
            part, dpart = scores[span], dprob[span]
            shifted = jnp.exp(part - jnp.max(part, axis=0, keepdims=True))
            prob = shifted * (1.0 / jnp.sum(shifted, axis=0, keepdims=True))
            proj = jnp.sum(prob * dpart, axis=0, keepdims=True)
            probs.append(prob.astype(BF16))
            steps.append((SCALE * prob * (dpart - proj)).astype(BF16))
        rounded, step = jnp.concatenate(probs, axis=0), jnp.concatenate(steps, axis=0)
        attended = nn(transposed_diag(v_lo[:, cols], v_hi[:, cols]), rounded).astype(BF16).T
        if len(out_refs) == 1:
            out_refs[0][:, cols] = attended
        else:
            tok_rows = attended.shape[0] // 2
            upper, lower = attended[:tok_rows], attended[tok_rows:]
            is_first = jnp.full(upper.shape, head_ref[0], jnp.int32) == 0
            out_refs[0][:, cols] = jnp.where(is_first, upper, lower)
            out_refs[1][:, cols] = jnp.where(is_first, lower, upper)
        dq_ref[:, cols] = nn(transposed_diag(k_lo[:, cols], k_hi[:, cols]), step).astype(BF16).T
        half = rows // 2
        for index, part in enumerate((join_pair(nn(step, queries)), join_pair(nn(rounded, grads)))):
            keep_ref[index, :, cols] = part[:half]
            send_ref[index, :, cols] = part[half:].astype(BF16)


def swap_lanes(x, shift):
    size = x.shape[-1]
    lane = lax.broadcasted_iota(jnp.int32, x.shape, x.ndim - 1)
    up = pltpu.roll(x, size - shift, x.ndim - 1)
    down = pltpu.roll(x, shift, x.ndim - 1)
    return jnp.where((lane & shift) == 0, up, down)


def merge_stats(mine, other, shift):
    other = swap_lanes(other, shift)
    top1, total1, mean1 = mine[0:2], mine[2:4], mine[4:6]
    top2, total2, mean2 = other[0:2], other[2:4], other[4:6]
    top = jnp.maximum(top1, top2)
    scale1, scale2 = jnp.exp(top1 - top), jnp.exp(top2 - top)
    part1, part2 = scale1 * total1, scale2 * total2
    total = part1 + part2
    mean = (part1 * mean1 + part2 * mean2) / jnp.where(total > 0.0, total, 1.0)
    shift1, shift2 = scale1 * (mean1 - mean), scale2 * (mean2 - mean)
    return top, total, mean, scale1, scale2, shift1, shift2


def stats_kernel(shift, mine_ref, other_ref, out_ref):
    for pair in range(mine_ref.shape[0]):
        top, total, mean = merge_stats(mine_ref[pair], other_ref[pair], shift)[:3]
        out_ref[pair] = jnp.concatenate([top, total, mean, jnp.zeros_like(top)], axis=0)


def merge_tables(pairs, factors):
    tables = []
    for pair in range(pairs):
        tables += factors(pair)
    table = jnp.concatenate(tables, axis=0)
    if table.shape[0] % 128:
        pad = jnp.zeros((-table.shape[0] % 128, table.shape[1]), F32)
        table = jnp.concatenate([table, pad], axis=0)
    return table.T


def weigh(table, pair, rows):
    low = first_head((rows, PAIR))
    at = pair * 8
    return [
        jnp.where(low, table[:rows, col : col + 1], table[:rows, col + 1 : col + 2])
        for col in (at, at + 2, at + 4, at + 6)
    ]


def audio_parts(table, pair, keep, recv):
    cols = pair_cols(pair)
    scale1, scale2, shift1, shift2 = weigh(table, pair, keep.shape[1])
    num1, step1, sum1 = (keep[index, :, cols] for index in range(3))
    num2, step2, sum2 = (recv[index, :, cols].astype(F32) for index in range(3))
    num = scale1 * num1 + scale2 * num2
    step = scale1 * step1 + shift1 * sum1 + scale2 * step2 + shift2 * sum2
    return num, step, scale1 * sum1 + scale2 * sum2


def spread_rows(part, outs, index, cols):
    rows = outs[0].shape[1]
    for slot, out in enumerate(outs):
        out[index, :, cols] = part[slot * rows : (slot + 1) * rows].astype(out.dtype)


def merge_audio_kernel(shift, mine_ref, other_ref, keep, recv, *outs):
    pairs = mine_ref.shape[0]
    table = merge_tables(
        pairs, lambda pair: list(merge_stats(mine_ref[pair], other_ref[pair], shift)[3:])
    )
    for pair in range(pairs):
        cols = pair_cols(pair)
        for index, part in enumerate(audio_parts(table, pair, keep, recv)):
            spread_rows(part, outs, index, cols)


def merge_video_kernel(keep, recv, *outs):
    for index in range(2):
        spread_rows(keep[index] + recv[index].astype(F32), outs, index, slice(None))


def settle_kernel(shift, mine_ref, other_ref, all_ref, keep_a, recv_a, keep_b, recv_b, *outs):
    pairs = mine_ref.shape[0]
    rows = outs[0].shape[1]

    def factors(pair):
        both = all_ref[pair]
        top, inverse, mean = both[0:2], 1.0 / both[2:4], both[4:6]
        mine, other = mine_ref[pair], swap_lanes(other_ref[pair], shift)
        scales = [jnp.exp(item[0:2] - top) * inverse for item in (mine, other)]
        return scales + [
            scale * (item[4:6] - mean) for scale, item in zip(scales, (mine, other))
        ]

    table = merge_tables(pairs, factors)
    for pair in range(pairs):
        cols = pair_cols(pair)
        num, step, _ = audio_parts(table, pair, keep_a, recv_a)
        key, val = (keep_b[index, :, cols] + recv_b[index, :, cols].astype(F32) for index in range(2))
        for index, part in enumerate((num, SCALE * step, key, val)):
            for slot, out in enumerate(outs):
                out[index, :, cols] = part[slot * rows : (slot + 1) * rows].astype(out.dtype)


def add_kernel(*refs):
    parts, outs = refs[:-4], refs[-4:]
    for index, out in enumerate(outs):
        total = parts[0][index].astype(F32)
        for part in parts[1:]:
            total = total + part[index].astype(F32)
        out[...] = total.astype(BF16)


def final_kernel(live_ref, q_lo, q_hi, c_lo, c_hi, key_ref, val_ref, stat_ref, dk_ref, dv_ref):
    for pair in range(stat_ref.shape[0]):
        cols = pair_cols(pair)
        keys, vals = key_ref[:, cols], val_ref[:, cols]
        queries = block_diag(q_lo[:, cols], q_hi[:, cols])
        cots = block_diag(c_lo[:, cols], c_hi[:, cols])
        stat = stat_ref[pair]
        top, inverse, mean = stat[0:2], 1.0 / stat[2:4], stat[4:6]
        top, inverse, mean = (
            jnp.concatenate([item[0:1], item[1:2]], axis=1) for item in (top, inverse, mean)
        )
        scores = nt(keys, queries) * SCALE
        live = lax.broadcasted_iota(jnp.int32, scores.shape, 0) < live_ref[0]
        probs = jnp.where(live, jnp.exp(scores - top), 0.0) * inverse
        dprob = nt(vals, cots)
        steps = (SCALE * probs * (dprob - mean)).astype(BF16)
        dk_ref[:, cols] = nn(steps, queries).astype(BF16)
        dv_ref[:, cols] = nn(probs.astype(BF16), cots).astype(BF16)


def pack_kernel(*refs):
    *inputs, packed, sems = refs
    width = inputs[0].shape[1]
    copies = [
        pltpu.make_async_copy(ref, packed.at[:, index * width : (index + 1) * width], sems.at[index])
        for index, ref in enumerate(inputs)
    ]
    for copy in copies:
        copy.start()
    for copy in copies:
        copy.wait()


def body(video_q, video_k, video_v, audio_q, audio_k, audio_v, video_length, video_cot, audio_cot):
    vid_rows, width = video_q.shape
    aud_rows = audio_q.shape[0]
    ctx_size, head_size = lax.axis_size("ctx"), lax.axis_size("head")
    ctx_index, head_index = lax.axis_index("ctx"), lax.axis_index("head")
    rows = aud_rows * ctx_size
    half = rows // 2
    pairs = width // PAIR
    group = min(GROUP, pairs)
    steps = pairs // group
    wide = group * PAIR
    bits = []
    while (1 << len(bits)) < ctx_size:
        bits.append(1 << len(bits))
    live = jnp.clip(video_length - ctx_index * vid_rows, 0, vid_rows).astype(jnp.int32)

    def flip(x, bit):
        return lax.ppermute(x, "ctx", [(i, i ^ bit) for i in range(ctx_size)])

    head_word = head_index.astype(jnp.int32)[None]
    scalar_spec = pl.BlockSpec(memory_space=pltpu.SMEM)
    cot = video_cot[0]
    tok_rows = cot.shape[0]
    if head_size == 2:
        sent = lax.dynamic_slice_in_dim(cot, (1 - head_index) * width, width, 1)
        kept = lax.dynamic_slice_in_dim(cot, head_index * width, width, 1)
        got = lax.ppermute(sent, "head", [(0, 1), (1, 0)])
        video_grad = jnp.concatenate(
            [jnp.where(head_index == 0, kept, got), jnp.where(head_index == 0, got, kept)], axis=0
        )
    else:
        video_grad = lax.all_to_all(cot, "head", split_axis=1, concat_axis=0, tiled=True)

    gathered = pl.pallas_call(
        pack_kernel,
        in_specs=[pl.BlockSpec(memory_space=pltpu.HBM)] * 4,
        out_specs=pl.BlockSpec(memory_space=pltpu.VMEM),
        out_shape=jax.ShapeDtypeStruct((aud_rows, 4 * width), BF16),
        scratch_shapes=[pltpu.SemaphoreType.DMA((4,))],
        name="pack",
    )(audio_q, audio_k, audio_v, audio_cot)
    quarters = [gathered]
    for bit in (bits[-1], bits[-2], bits[-1] | bits[-2]):
        quarters.append(flip(gathered, bit))
    gathered = jnp.concatenate(quarters, axis=0)
    for bit in reversed(bits[1:-2]):
        got_rows = flip(gathered, bit)
        gathered = jnp.concatenate([gathered, got_rows], axis=0)
    halves = (gathered, flip(gathered, bits[0]))

    def audio_spec(which):
        return pl.BlockSpec((half, wide), lambda step: (0, which * steps + step))

    vid_spec = pl.BlockSpec((vid_rows, wide), lambda step: (0, step))
    stat_spec = pl.BlockSpec((group, 8, rows), lambda step: (step, 0, 0))
    stat_shape = jax.ShapeDtypeStruct((pairs, 8, rows), F32)

    def part_spec(count):
        return pl.BlockSpec((count, half, wide), lambda step: (0, 0, step))

    def part_shapes(count, part_rows):
        return [
            jax.ShapeDtypeStruct((count, part_rows, width), F32),
            jax.ShapeDtypeStruct((count, part_rows, width), BF16),
        ]

    product = 2 * vid_rows * 2 * rows * PAIR * pairs
    vid_bytes = 2 * vid_rows * width
    vid_shape = jax.ShapeDtypeStruct((vid_rows, width), BF16)

    def cost(matmuls, moved):
        return pl.CostEstimate(
            flops=matmuls * product, bytes_accessed=moved * vid_bytes, transcendentals=vid_rows * 2 * rows * pairs
        )

    stats, keep_a, send_a = pl.pallas_call(
        audio_kernel,
        grid=(steps,),
        compiler_params=PARAMS,
        in_specs=[scalar_spec, audio_spec(0), audio_spec(0), audio_spec(3), audio_spec(3), vid_spec, vid_spec],
        out_specs=[stat_spec, part_spec(3), part_spec(3)],
        out_shape=[stat_shape, *part_shapes(3, half)],
        cost_estimate=cost(5, 5),
        name="audio_side",
    )(live, *halves, *halves, video_k, video_v)

    if head_size == 2:
        tok_spec = pl.BlockSpec((tok_rows, wide), lambda step: (0, step))
        out_specs = [tok_spec, tok_spec]
        out_shapes = [jax.ShapeDtypeStruct((tok_rows, width), BF16)] * 2
    else:
        out_specs, out_shapes = [vid_spec], [vid_shape]
    *attended, grad_video_q, keep_b, send_b = pl.pallas_call(
        video_kernel,
        grid=(steps,),
        compiler_params=PARAMS,
        in_specs=[scalar_spec, audio_spec(1), audio_spec(1), audio_spec(2), audio_spec(2), vid_spec, vid_spec],
        out_specs=[*out_specs, vid_spec, part_spec(2), part_spec(2)],
        out_shape=[*out_shapes, vid_shape, *part_shapes(2, half)],
        cost_estimate=cost(6, 6),
        name="video_side",
    )(head_word, *halves, *halves, video_q, video_grad)

    if head_size == 2:
        mine, theirs = attended
        other = lax.ppermute(theirs, "head", [(0, 1), (1, 0)])
        video_out = jnp.concatenate(
            [jnp.where(head_index == 0, mine, other), jnp.where(head_index == 0, other, mine)], axis=1
        )[None]
    else:
        video_out = lax.all_to_all(attended[0], "head", split_axis=0, concat_axis=1, tiled=True)[None]

    part_rows = half
    high, low = bits[-1], bits[-2]
    exchanges = tuple(zip((high, low, high | low), range(1, 4)))
    for level, bit in enumerate(bits[:-2]):
        other = flip(stats, bit)
        recv_a = flip(send_a, bit)
        recv_b = flip(send_b, bit)
        merged_stats = pl.pallas_call(
            functools.partial(stats_kernel, part_rows), out_shape=stat_shape, compiler_params=PARAMS
        )(stats, other)
        if level < len(bits) - 3:
            keep_a, send_a = pl.pallas_call(
                functools.partial(merge_audio_kernel, part_rows),
                out_shape=part_shapes(3, part_rows // 2),
                compiler_params=PARAMS,
            )(stats, other, keep_a, recv_a)
            keep_b, send_b = pl.pallas_call(
                merge_video_kernel, out_shape=part_shapes(2, part_rows // 2), compiler_params=PARAMS
            )(keep_b, recv_b)
            stats = merged_stats
            part_rows //= 2
        else:
            final_stats = merged_stats
            for step_bit, shift in ((low, 2 * aud_rows), (high, aud_rows)):
                step_other = flip(final_stats, step_bit)
                final_stats = pl.pallas_call(
                    functools.partial(stats_kernel, shift), out_shape=stat_shape, compiler_params=PARAMS
                )(final_stats, step_other)
            slots = pl.pallas_call(
                functools.partial(settle_kernel, part_rows),
                out_shape=[jax.ShapeDtypeStruct((4, aud_rows, width), dtype) for dtype in (F32, BF16, BF16, BF16)],
                compiler_params=PARAMS,
                name="settle",
            )(stats, other, final_stats, keep_a, recv_a, keep_b, recv_b)
    parts = [slots[0]]
    for step_bit, slot in exchanges:
        parts.append(flip(slots[slot], step_bit))
    audio_out, grad_audio_q, grad_audio_k, grad_audio_v = pl.pallas_call(
        add_kernel,
        out_shape=[jax.ShapeDtypeStruct((aud_rows, width), BF16)] * 4,
        compiler_params=PARAMS,
        name="add",
    )(*parts)

    grad_video_k, grad_video_v = pl.pallas_call(
        final_kernel,
        grid=(steps,),
        compiler_params=PARAMS,
        in_specs=[
            scalar_spec,
            audio_spec(0),
            audio_spec(0),
            audio_spec(3),
            audio_spec(3),
            vid_spec,
            vid_spec,
            stat_spec,
        ],
        out_specs=[vid_spec, vid_spec],
        out_shape=[vid_shape, vid_shape],
        cost_estimate=cost(4, 4),
        name="audio_grads",
    )(live, *halves, *halves, video_k, video_v, final_stats)
    return (
        video_out,
        audio_out,
        grad_video_q,
        grad_video_k,
        grad_video_v,
        grad_audio_q,
        grad_audio_k,
        grad_audio_v,
    )


def solution(mesh):
    wide = P("ctx", "head")
    tall = P("ctx", "head", None)

    return jax.shard_map(
        body,
        mesh=mesh,
        in_specs=(wide, wide, wide, wide, wide, wide, P(), tall, wide),
        out_specs=(tall, wide, wide, wide, wide, wide, wide, wide),
        check_vma=False,
    )
```

```python
import functools

import jax
import jax.numpy as jnp
from jax import lax
from jax.experimental import pallas as pl
from jax.experimental.pallas import tpu as pltpu
from jax.sharding import PartitionSpec as P


HEAD_DIM = 64
PAIR = 2 * HEAD_DIM
SCALE = HEAD_DIM ** (-0.5)
NEG = -1e30
GROUP = 8
PARAMS = pltpu.CompilerParams(vmem_limit_bytes=20 * 1024 * 1024)
F32 = jnp.float32
BF16 = jnp.bfloat16


def nt(x, y):
    return lax.dot_general(x, y, (((1,), (1,)), ((), ())), preferred_element_type=F32)


def nn(x, y):
    return jnp.dot(x, y, preferred_element_type=F32)


def first_head(shape):
    return lax.broadcasted_iota(jnp.int32, shape, len(shape) - 1) < HEAD_DIM


def block_diag(refs, cols):
    rows = jnp.concatenate([ref[:, cols] for ref in refs], axis=0)
    keep = first_head(rows.shape)
    zero = jnp.zeros_like(rows)
    return jnp.concatenate([jnp.where(keep, rows, zero), jnp.where(keep, zero, rows)], axis=0)


def join_pair(stacked):
    rows = stacked.shape[0] // 2
    return jnp.where(first_head((rows, PAIR)), stacked[:rows], stacked[rows:])


def pair_cols(pair):
    return slice(pair * PAIR, (pair + 1) * PAIR)


def audio_kernel(live_ref, *refs):
    q_refs, c_refs = refs[:4], refs[4:8]
    key_ref, val_ref, stat_ref, keep_ref, send_ref = refs[8:]
    for pair in range(stat_ref.shape[1] // 2):
        cols = pair_cols(pair)
        keys, vals = key_ref[:, cols], val_ref[:, cols]
        queries = block_diag(q_refs, cols)
        cots = block_diag(c_refs, cols)
        rows = queries.shape[0] // 2
        scores = nt(queries, keys) * SCALE
        live = lax.broadcasted_iota(jnp.int32, scores.shape, 1) < live_ref[0]
        top = jnp.max(jnp.where(live, scores, NEG), axis=1, keepdims=True)
        weights = jnp.where(live, jnp.exp(scores - top), 0.0)
        total = jnp.sum(weights, axis=1, keepdims=True)
        dprob = nt(cots, vals)
        mean = jnp.sum(weights * dprob, axis=1, keepdims=True) / jnp.where(total > 0.0, total, 1.0)
        spread = (weights * (dprob - mean)).astype(BF16)
        rounded = weights.astype(BF16)
        parts = (
            join_pair(nn(rounded, vals)),
            join_pair(nn(spread, keys)),
            join_pair(nn(rounded, keys)),
        )
        half = rows // 2
        for index, part in enumerate(parts):
            keep_ref[index, :, cols] = part[:half]
            send_ref[index, :, cols] = part[half:].astype(BF16)
        lane = lax.broadcasted_iota(jnp.int32, (rows, PAIR), 1)
        table = jnp.zeros((rows, PAIR), F32)
        for index, column in enumerate((top, total, mean)):
            table = jnp.where(lane == 2 * index, column[:rows], table)
            table = jnp.where(lane == 2 * index + 1, column[rows:], table)
        turned = table.T
        for index in range(3):
            stat_ref[index, 2 * pair : 2 * pair + 2] = turned[2 * index : 2 * index + 2]


def transposed_diag(refs, cols):
    turned = jnp.concatenate([ref[:, cols] for ref in refs], axis=0).T
    keep = lax.broadcasted_iota(jnp.int32, turned.shape, 0) < HEAD_DIM
    zero = jnp.zeros_like(turned)
    return jnp.concatenate([jnp.where(keep, turned, zero), jnp.where(keep, zero, turned)], axis=1)


def video_kernel(head_ref, *refs):
    k_refs, v_refs, (query_ref, grad_ref), outs = refs[:4], refs[4:8], refs[8:10], refs[10:]
    *out_refs, dq_ref, keep_ref, send_ref = outs
    for pair in range(query_ref.shape[1] // PAIR):
        cols = pair_cols(pair)
        queries, grads = query_ref[:, cols], grad_ref[:, cols]
        keys = block_diag(k_refs, cols)
        vals = block_diag(v_refs, cols)
        rows = keys.shape[0] // 2
        scores = nt(keys, queries) * SCALE
        dprob = nt(vals, grads)
        probs, steps = [], []
        for head in range(2):
            span = slice(head * rows, (head + 1) * rows)
            part, dpart = scores[span], dprob[span]
            shifted = jnp.exp(part - jnp.max(part, axis=0, keepdims=True))
            prob = shifted * (1.0 / jnp.sum(shifted, axis=0, keepdims=True))
            proj = jnp.sum(prob * dpart, axis=0, keepdims=True)
            probs.append(prob.astype(BF16))
            steps.append((SCALE * prob * (dpart - proj)).astype(BF16))
        rounded, step = jnp.concatenate(probs, axis=0), jnp.concatenate(steps, axis=0)
        attended = nn(transposed_diag(v_refs, cols), rounded).astype(BF16).T
        if len(out_refs) == 1:
            out_refs[0][:, cols] = attended
        else:
            tok_rows = attended.shape[0] // 2
            upper, lower = attended[:tok_rows], attended[tok_rows:]
            is_first = jnp.full(upper.shape, head_ref[0], jnp.int32) == 0
            out_refs[0][:, cols] = jnp.where(is_first, upper, lower)
            out_refs[1][:, cols] = jnp.where(is_first, lower, upper)
        dq_ref[:, cols] = nn(transposed_diag(k_refs, cols), step).astype(BF16).T
        half = rows // 2
        for index, part in enumerate((join_pair(nn(step, queries)), join_pair(nn(rounded, grads)))):
            keep_ref[index, :, cols] = part[:half]
            send_ref[index, :, cols] = part[half:].astype(BF16)


def swap_lanes(x, shift):
    size = x.shape[-1]
    lane = lax.broadcasted_iota(jnp.int32, x.shape, x.ndim - 1)
    up = pltpu.roll(x, size - shift, x.ndim - 1)
    down = pltpu.roll(x, shift, x.ndim - 1)
    return jnp.where((lane & shift) == 0, up, down)


def merge_stats(mine_ref, other_ref, shift):
    top1, total1, mean1 = (mine_ref[index] for index in range(3))
    top2, total2, mean2 = (swap_lanes(other_ref[index], shift) for index in range(3))
    top = jnp.maximum(top1, top2)
    scale1, scale2 = jnp.exp(top1 - top), jnp.exp(top2 - top)
    part1, part2 = scale1 * total1, scale2 * total2
    total = part1 + part2
    mean = (part1 * mean1 + part2 * mean2) / jnp.where(total > 0.0, total, 1.0)
    shift1, shift2 = scale1 * (mean1 - mean), scale2 * (mean2 - mean)
    return (top, total, mean), (scale1, scale2, shift1, shift2)


def stats_kernel(shift, mine_ref, other_ref, out_ref):
    for index, item in enumerate(merge_stats(mine_ref, other_ref, shift)[0]):
        out_ref[index] = item


def factor_table(factors):
    table = jnp.concatenate(factors, axis=0)
    if table.shape[0] % 128:
        pad = jnp.zeros((-table.shape[0] % 128, table.shape[1]), F32)
        table = jnp.concatenate([table, pad], axis=0)
    return table.T


def kept_rows(table, count):
    far = table.shape[0] // 4
    return jnp.concatenate([table[: count // 2], table[far : far + count // 2]], axis=0)


def weigh(table, pair, heads):
    low = first_head((table.shape[0], PAIR))
    return [
        jnp.where(low, table[:, col : col + 1], table[:, col + 1 : col + 2])
        for col in range(2 * pair, 4 * heads, heads)
    ]


def audio_parts(table, pair, heads, keep, recv):
    cols = pair_cols(pair)
    scale1, scale2, shift1, shift2 = weigh(table, pair, heads)
    num1, step1, sum1 = (keep[index, :, cols] for index in range(3))
    num2, step2, sum2 = (recv[index, :, cols].astype(F32) for index in range(3))
    num = scale1 * num1 + scale2 * num2
    step = scale1 * step1 + shift1 * sum1 + scale2 * step2 + shift2 * sum2
    return num, step, scale1 * sum1 + scale2 * sum2


def split_rows(part, keep_ref, send_ref, index, cols):
    size = part.shape[0] // 4
    for piece in range(2):
        rows = slice(piece * size, (piece + 1) * size)
        keep_ref[index, rows, cols] = part[2 * piece * size : (2 * piece + 1) * size]
        send_ref[index, rows, cols] = part[(2 * piece + 1) * size : (2 * piece + 2) * size].astype(BF16)


def merge_audio_kernel(shift, mine_ref, other_ref, keep, recv, keep_ref, send_ref):
    heads = mine_ref.shape[1]
    table = kept_rows(factor_table(merge_stats(mine_ref, other_ref, shift)[1]), keep.shape[1])
    for pair in range(heads // 2):
        cols = pair_cols(pair)
        for index, part in enumerate(audio_parts(table, pair, heads, keep, recv)):
            split_rows(part, keep_ref, send_ref, index, cols)


def merge_video_kernel(keep, recv, keep_ref, send_ref):
    for index in range(2):
        split_rows(keep[index] + recv[index].astype(F32), keep_ref, send_ref, index, slice(None))


def settle_kernel(shift, mine_ref, other_ref, all_ref, keep_a, recv_a, keep_b, recv_b, *outs):
    heads = mine_ref.shape[1]
    rows = outs[0].shape[1]
    top, inverse, mean = all_ref[0], 1.0 / all_ref[1], all_ref[2]
    mine = [mine_ref[0], mine_ref[2]]
    other = [swap_lanes(other_ref[0], shift), swap_lanes(other_ref[2], shift)]
    scales = [jnp.exp(item[0] - top) * inverse for item in (mine, other)]
    shifts = [scale * (item[1] - mean) for scale, item in zip(scales, (mine, other))]
    table = kept_rows(factor_table(scales + shifts), keep_a.shape[1])
    for pair in range(heads // 2):
        cols = pair_cols(pair)
        num, step, _ = audio_parts(table, pair, heads, keep_a, recv_a)
        key, val = (keep_b[index, :, cols] + recv_b[index, :, cols].astype(F32) for index in range(2))
        for index, part in enumerate((num, SCALE * step, key, val)):
            for slot, out in enumerate(outs):
                out[index, :, cols] = part[slot * rows : (slot + 1) * rows].astype(out.dtype)


def add_kernel(*refs):
    parts, outs = refs[:-4], refs[-4:]
    for index, out in enumerate(outs):
        total = parts[0][index].astype(F32)
        for part in parts[1:]:
            total = total + part[index].astype(F32)
        out[...] = total.astype(BF16)


def final_kernel(live_ref, *refs):
    q_refs, c_refs = refs[:4], refs[4:8]
    key_ref, val_ref, stat_ref, dk_ref, dv_ref = refs[8:]
    for pair in range(stat_ref.shape[1] // 2):
        cols = pair_cols(pair)
        keys, vals = key_ref[:, cols], val_ref[:, cols]
        queries = block_diag(q_refs, cols)
        cots = block_diag(c_refs, cols)
        top, total, mean = (
            jnp.concatenate(
                [stat_ref[index, row : row + 1] for row in (2 * pair, 2 * pair + 1)], axis=1
            )
            for index in range(3)
        )
        inverse = 1.0 / total
        scores = nt(keys, queries) * SCALE
        live = lax.broadcasted_iota(jnp.int32, scores.shape, 0) < live_ref[0]
        probs = jnp.where(live, jnp.exp(scores - top), 0.0) * inverse
        dprob = nt(vals, cots)
        steps = (SCALE * probs * (dprob - mean)).astype(BF16)
        dk_ref[:, cols] = nn(steps, queries).astype(BF16)
        dv_ref[:, cols] = nn(probs.astype(BF16), cots).astype(BF16)


def pack_kernel(*refs):
    *inputs, packed, sems = refs
    width = inputs[0].shape[1]
    copies = [
        pltpu.make_async_copy(ref, packed.at[:, index * width : (index + 1) * width], sems.at[index])
        for index, ref in enumerate(inputs)
    ]
    for copy in copies:
        copy.start()
    for copy in copies:
        copy.wait()


def body(video_q, video_k, video_v, audio_q, audio_k, audio_v, video_length, video_cot, audio_cot):
    vid_rows, width = video_q.shape
    aud_rows = audio_q.shape[0]
    ctx_size, head_size = lax.axis_size("ctx"), lax.axis_size("head")
    ctx_index, head_index = lax.axis_index("ctx"), lax.axis_index("head")
    rows = aud_rows * ctx_size
    half = rows // 2
    pairs = width // PAIR
    group = min(GROUP, pairs)
    steps = pairs // group
    wide = group * PAIR
    bits = []
    while (1 << len(bits)) < ctx_size:
        bits.append(1 << len(bits))
    live = jnp.clip(video_length - ctx_index * vid_rows, 0, vid_rows).astype(jnp.int32)

    def flip(x, bit):
        return lax.ppermute(x, "ctx", [(i, i ^ bit) for i in range(ctx_size)])

    head_word = head_index.astype(jnp.int32)[None]
    scalar_spec = pl.BlockSpec(memory_space=pltpu.SMEM)
    cot = video_cot[0]
    tok_rows = cot.shape[0]
    if head_size == 2:
        sent = lax.dynamic_slice_in_dim(cot, (1 - head_index) * width, width, 1)
        kept = lax.dynamic_slice_in_dim(cot, head_index * width, width, 1)
        got = lax.ppermute(sent, "head", [(0, 1), (1, 0)])
        video_grad = jnp.concatenate(
            [jnp.where(head_index == 0, kept, got), jnp.where(head_index == 0, got, kept)], axis=0
        )
    else:
        video_grad = lax.all_to_all(cot, "head", split_axis=1, concat_axis=0, tiled=True)

    gathered = pl.pallas_call(
        pack_kernel,
        in_specs=[pl.BlockSpec(memory_space=pltpu.HBM)] * 4,
        out_specs=pl.BlockSpec(memory_space=pltpu.VMEM),
        out_shape=jax.ShapeDtypeStruct((aud_rows, 4 * width), BF16),
        scratch_shapes=[pltpu.SemaphoreType.DMA((4,))],
        name="pack",
    )(audio_q, audio_cot, audio_k, audio_v)
    high, low = bits[-1], bits[-2]

    def across(held):
        for bit in reversed(bits[1:-2]):
            held = jnp.concatenate([held, flip(held, bit)], axis=0)
        return held, flip(held, bits[0])

    distant = flip(gathered, high), flip(gathered, high | low)
    near = across(jnp.concatenate([gathered, flip(gathered, low)], axis=0))
    joined_a = jnp.concatenate([part[:, : 2 * width] for part in distant], axis=0)
    joined_b = jnp.concatenate([part[:, 2 * width :] for part in distant], axis=0)
    far_a, far_b = across(joined_a), across(joined_b)
    asked = (near[0], far_a[0], near[1], far_a[1])
    given = (near[0], far_b[0], near[1], far_b[1])

    def audio_specs(which):
        near_spec, far_spec = (
            pl.BlockSpec((rows // 4, wide), lambda step, at=at: (0, at * steps + step))
            for at in (which, which % 2)
        )
        return [near_spec, far_spec] * 2

    vid_spec = pl.BlockSpec((vid_rows, wide), lambda step: (0, step))
    stat_spec = pl.BlockSpec((3, 2 * group, rows), lambda step: (0, step, 0))
    stat_shape = jax.ShapeDtypeStruct((3, 2 * pairs, rows), F32)

    def part_spec(count):
        return pl.BlockSpec((count, half, wide), lambda step: (0, 0, step))

    def part_shapes(count, part_rows):
        return [
            jax.ShapeDtypeStruct((count, part_rows, width), F32),
            jax.ShapeDtypeStruct((count, part_rows, width), BF16),
        ]

    product = 2 * vid_rows * 2 * rows * PAIR * pairs
    vid_bytes = 2 * vid_rows * width
    vid_shape = jax.ShapeDtypeStruct((vid_rows, width), BF16)

    def cost(matmuls, moved):
        return pl.CostEstimate(
            flops=matmuls * product, bytes_accessed=moved * vid_bytes, transcendentals=vid_rows * 2 * rows * pairs
        )

    stats, keep_a, send_a = pl.pallas_call(
        audio_kernel,
        grid=(steps,),
        compiler_params=PARAMS,
        in_specs=[scalar_spec, *audio_specs(0), *audio_specs(1), vid_spec, vid_spec],
        out_specs=[stat_spec, part_spec(3), part_spec(3)],
        out_shape=[stat_shape, *part_shapes(3, half)],
        cost_estimate=cost(5, 5),
        name="audio_side",
    )(live, *asked, *asked, video_k, video_v)

    if head_size == 2:
        tok_spec = pl.BlockSpec((tok_rows, wide), lambda step: (0, step))
        out_specs = [tok_spec, tok_spec]
        out_shapes = [jax.ShapeDtypeStruct((tok_rows, width), BF16)] * 2
    else:
        out_specs, out_shapes = [vid_spec], [vid_shape]
    *attended, grad_video_q, keep_b, send_b = pl.pallas_call(
        video_kernel,
        grid=(steps,),
        compiler_params=PARAMS,
        in_specs=[scalar_spec, *audio_specs(2), *audio_specs(3), vid_spec, vid_spec],
        out_specs=[*out_specs, vid_spec, part_spec(2), part_spec(2)],
        out_shape=[*out_shapes, vid_shape, *part_shapes(2, half)],
        cost_estimate=cost(6, 6),
        name="video_side",
    )(head_word, *given, *given, video_q, video_grad)

    if head_size == 2:
        mine, theirs = attended
        other = lax.ppermute(theirs, "head", [(0, 1), (1, 0)])
        video_out = jnp.concatenate(
            [jnp.where(head_index == 0, mine, other), jnp.where(head_index == 0, other, mine)], axis=1
        )[None]
    else:
        video_out = lax.all_to_all(attended[0], "head", split_axis=0, concat_axis=1, tiled=True)[None]

    part_rows, shift = half, half
    exchanges = tuple(zip((low, high, high | low), range(1, 4)))
    for level, bit in enumerate(bits[:-2]):
        other = flip(stats, bit)
        recv_a = flip(send_a, bit)
        recv_b = flip(send_b, bit)
        merged_stats = pl.pallas_call(
            functools.partial(stats_kernel, shift), out_shape=stat_shape, compiler_params=PARAMS
        )(stats, other)
        if level < len(bits) - 3:
            keep_a, send_a = pl.pallas_call(
                functools.partial(merge_audio_kernel, shift),
                out_shape=part_shapes(3, part_rows // 2),
                compiler_params=PARAMS,
            )(stats, other, keep_a, recv_a)
            keep_b, send_b = pl.pallas_call(
                merge_video_kernel, out_shape=part_shapes(2, part_rows // 2), compiler_params=PARAMS
            )(keep_b, recv_b)
            stats = merged_stats
            part_rows //= 2
            shift = part_rows // 2
        else:
            final_stats = merged_stats
            for step_bit, step_shift in ((low, aud_rows), (high, half // 2)):
                step_other = flip(final_stats, step_bit)
                final_stats = pl.pallas_call(
                    functools.partial(stats_kernel, step_shift), out_shape=stat_shape, compiler_params=PARAMS
                )(final_stats, step_other)
            slots = pl.pallas_call(
                functools.partial(settle_kernel, shift),
                out_shape=[jax.ShapeDtypeStruct((4, aud_rows, width), dtype) for dtype in (F32, BF16, BF16, BF16)],
                compiler_params=PARAMS,
                name="settle",
            )(stats, other, final_stats, keep_a, recv_a, keep_b, recv_b)
    parts = [slots[0]]
    for step_bit, slot in exchanges:
        parts.append(flip(slots[slot], step_bit))
    audio_out, grad_audio_q, grad_audio_k, grad_audio_v = pl.pallas_call(
        add_kernel,
        out_shape=[jax.ShapeDtypeStruct((aud_rows, width), BF16)] * 4,
        compiler_params=PARAMS,
        name="add",
    )(*parts)

    grad_video_k, grad_video_v = pl.pallas_call(
        final_kernel,
        grid=(steps,),
        compiler_params=PARAMS,
        in_specs=[
            scalar_spec,
            *audio_specs(0),
            *audio_specs(1),
            vid_spec,
            vid_spec,
            stat_spec,
        ],
        out_specs=[vid_spec, vid_spec],
        out_shape=[vid_shape, vid_shape],
        cost_estimate=cost(4, 4),
        name="audio_grads",
    )(live, *asked, *asked, video_k, video_v, final_stats)
    return (
        video_out,
        audio_out,
        grad_video_q,
        grad_video_k,
        grad_video_v,
        grad_audio_q,
        grad_audio_k,
        grad_audio_v,
    )


def solution(mesh):
    wide = P("ctx", "head")
    tall = P("ctx", "head", None)

    return jax.shard_map(
        body,
        mesh=mesh,
        in_specs=(wide, wide, wide, wide, wide, wide, P(), tall, wide),
        out_specs=(tall, wide, wide, wide, wide, wide, wide, wide),
        check_vma=False,
    )
```
